64 devices in a mesh: dp: 4 (over x, y), sp: 16 (over z, core).
Axes of the slice: x: 2, y: 2, z: 8, core: 2. Of those that a mesh axis runs over, the one named last changes fastest.
The devices are a block of a 4x4x8 slice.
Arguments:
- tok_in: bfloat16 [8192, 5120], P(('dp', 'sp')), parts along dimension 0
- tok_pos: int32 [8192], P(('dp', 'sp')), parts along dimension 0
- w_dq: bfloat16 [5120, 1536], replicated
- g_q: float32 [1536], replicated
- w_uq: bfloat16 [1536, 128, 192], replicated
- w_dkv: bfloat16 [5120, 576], replicated
- g_kv: float32 [512], replicated
- w_uk: bfloat16 [512, 128, 128], replicated
- w_uv: bfloat16 [512, 128, 128], replicated
- w_o: bfloat16 [128, 128, 5120], replicated
Outputs:
- output 1: bfloat16 [8192, 5120], P(('dp', 'sp')), parts along dimension 0
- output 2: bfloat16 [8192, 512], P(('dp', 'sp')), parts along dimension 0
- output 3: bfloat16 [8192, 64], P(('dp', 'sp')), parts along dimension 0
There are 4 independent parts. The reference program is written for one: setup_inputs(seed, part) draws one part's arguments, and reference() takes and returns one part's arrays. A program takes and returns all parts, laid end to end along the dimension named above; an argument that names none is the same for every part.
All inputs are finite; a program needn't handle non-finite values.
Results may differ from the reference program's by a relative error of at most 0.0063.
Values are sent between devices in bfloat16 or wider.
A program may use at most 768 MiB of HBM per device.

```python
import math
import jax
import jax.numpy as jnp
from jax import lax

SEQ_LEN = 2048
ROW_BLOCK = 128
MODEL_DIM = 5120
NUM_HEADS = 128
Q_RANK = 1536
KV_RANK = 512
NOPE_DIM = 128
ROPE_DIM = 64
V_DIM = 128

ROPE_THETA = 10000.0
YARN_FACTOR = 40.0
ORIG_CTX = 4096.0
BETA_FAST = 32.0
BETA_SLOW = 1.0
NORM_EPS = 1e-6


def rope_freqs(rot_dim):
    half_dim = rot_dim // 2
    log_base = 2.0 * math.log(ROPE_THETA)
    low_idx = max(math.floor(rot_dim * math.log(ORIG_CTX / (BETA_FAST * 2.0 * math.pi)) / log_base), 0)
    high_idx = min(math.ceil(rot_dim * math.log(ORIG_CTX / (BETA_SLOW * 2.0 * math.pi)) / log_base), half_dim - 1)
    spread = max(high_idx - low_idx, 0.001)
    freq_list = []
    for freq_idx in range(half_dim):
        base_freq = ROPE_THETA ** (-2.0 * freq_idx / rot_dim)
        ramp_val = min(max((freq_idx - low_idx) / spread, 0.0), 1.0)
        freq_list.append(base_freq / YARN_FACTOR * ramp_val + base_freq * (1.0 - ramp_val))
    return jnp.asarray(freq_list, dtype=jnp.float32)


def rotate_half(act_in, cos_t, sin_t):
    half_dim = act_in.shape[-1] // 2
    first = act_in[..., :half_dim]
    second = act_in[..., half_dim:]
    return jnp.concatenate([first * cos_t - second * sin_t, second * cos_t + first * sin_t], axis=-1)


def rms_norm(act_in, gain):
    mean_sq = jnp.mean(act_in * act_in, axis=-1, keepdims=True)
    return act_in * lax.rsqrt(mean_sq + NORM_EPS) * gain


def setup_inputs(seed: int = 0, part: int = 0) -> dict:
    root_key = jax.random.key(seed)
    part_key = jax.random.fold_in(root_key, part)
    key_x, key_pos = jax.random.split(part_key)
    weight_keys = jax.random.split(root_key, 8)

    def draw_weight(sub_key, arr_shape, fan_in):
        return (jax.random.normal(sub_key, arr_shape, jnp.float32) * fan_in ** -0.5).astype(jnp.bfloat16)

    tok_in = jax.random.normal(key_x, (SEQ_LEN, MODEL_DIM), jnp.float32).astype(jnp.bfloat16)
    pos_steps = jax.random.randint(key_pos, (SEQ_LEN,), 1, 5, dtype=jnp.int32)
    tok_pos = (jnp.cumsum(pos_steps) - pos_steps[0]).astype(jnp.int32)
    w_dq = draw_weight(weight_keys[0], (MODEL_DIM, Q_RANK), MODEL_DIM)
    g_q = jax.random.uniform(weight_keys[1], (Q_RANK,), jnp.float32, 0.5, 1.5)
    w_uq = draw_weight(weight_keys[2], (Q_RANK, NUM_HEADS, NOPE_DIM + ROPE_DIM), Q_RANK)
    w_dkv = draw_weight(weight_keys[3], (MODEL_DIM, KV_RANK + ROPE_DIM), MODEL_DIM)
    g_kv = jax.random.uniform(weight_keys[4], (KV_RANK,), jnp.float32, 0.5, 1.5)
    w_uk = draw_weight(weight_keys[5], (KV_RANK, NUM_HEADS, NOPE_DIM), KV_RANK)
    w_uv = draw_weight(weight_keys[6], (KV_RANK, NUM_HEADS, V_DIM), KV_RANK)
    w_o = draw_weight(weight_keys[7], (NUM_HEADS, V_DIM, MODEL_DIM), NUM_HEADS * V_DIM)
    return dict(tok_in=tok_in, tok_pos=tok_pos, w_dq=w_dq, g_q=g_q, w_uq=w_uq, w_dkv=w_dkv, g_kv=g_kv, w_uk=w_uk, w_uv=w_uv, w_o=w_o)


def reference(tok_in, tok_pos, w_dq, g_q, w_uq, w_dkv, g_kv, w_uk, w_uv, w_o):
    qk_dim = NOPE_DIM + ROPE_DIM
    attn_scale = (0.1 * math.log(YARN_FACTOR) + 1.0) ** 2 / math.sqrt(qk_dim)
    angles = tok_pos.astype(jnp.float32)[:, None] * rope_freqs(ROPE_DIM)[None, :]
    cos_t = jnp.cos(angles)
    sin_t = jnp.sin(angles)
    q_lat = rms_norm(jnp.dot(tok_in, w_dq, preferred_element_type=jnp.float32), g_q).astype(jnp.bfloat16)
    q_full = jnp.dot(q_lat, w_uq.reshape(Q_RANK, NUM_HEADS * qk_dim), preferred_element_type=jnp.float32).reshape(SEQ_LEN, NUM_HEADS, qk_dim)
    q_nope = q_full[:, :, :NOPE_DIM].astype(jnp.bfloat16)
    q_rot = rotate_half(q_full[:, :, NOPE_DIM:], cos_t[:, None, :], sin_t[:, None, :]).astype(jnp.bfloat16)
    kv_lat = jnp.dot(tok_in, w_dkv, preferred_element_type=jnp.float32)
    cache_kv = rms_norm(kv_lat[:, :KV_RANK], g_kv).astype(jnp.bfloat16)
    cache_pe = rotate_half(kv_lat[:, KV_RANK:], cos_t, sin_t).astype(jnp.bfloat16)
    k_nope = jnp.dot(cache_kv, w_uk.reshape(KV_RANK, NUM_HEADS * NOPE_DIM), preferred_element_type=jnp.float32).reshape(SEQ_LEN, NUM_HEADS, NOPE_DIM).astype(jnp.bfloat16)
    values = jnp.dot(cache_kv, w_uv.reshape(KV_RANK, NUM_HEADS * V_DIM), preferred_element_type=jnp.float32).reshape(SEQ_LEN, NUM_HEADS, V_DIM).astype(jnp.bfloat16)
    key_idx = jnp.arange(SEQ_LEN)
    num_blocks = SEQ_LEN // ROW_BLOCK

    def head_attention(head_in):
        qn_head, qr_head, kn_head, v_head = head_in

        def block_attention(blk_idx):
            start = blk_idx * ROW_BLOCK
            qn_blk = lax.dynamic_slice_in_dim(qn_head, start, ROW_BLOCK, axis=0)
            qr_blk = lax.dynamic_slice_in_dim(qr_head, start, ROW_BLOCK, axis=0)
            logits = jnp.dot(qn_blk, kn_head.T, preferred_element_type=jnp.float32) + jnp.dot(qr_blk, cache_pe.T, preferred_element_type=jnp.float32)
            logits = logits * attn_scale
            row_idx = start + jnp.arange(ROW_BLOCK)
            logits = jnp.where(key_idx[None, :] <= row_idx[:, None], logits, -jnp.inf)
            attn_prob = jax.nn.softmax(logits, axis=-1).astype(jnp.bfloat16)
            return jnp.dot(attn_prob, v_head, preferred_element_type=jnp.float32).astype(jnp.bfloat16)

        return lax.map(block_attention, jnp.arange(num_blocks)).reshape(SEQ_LEN, V_DIM)

    head_outs = lax.map(head_attention, (jnp.swapaxes(q_nope, 0, 1), jnp.swapaxes(q_rot, 0, 1), jnp.swapaxes(k_nope, 0, 1), jnp.swapaxes(values, 0, 1)))
    attn_cat = jnp.swapaxes(head_outs, 0, 1).reshape(SEQ_LEN, NUM_HEADS * V_DIM)
    attn_out = jnp.dot(attn_cat, w_o.reshape(NUM_HEADS * V_DIM, MODEL_DIM), preferred_element_type=jnp.float32).astype(jnp.bfloat16)
    return attn_out, cache_kv, cache_pe
```

```python
import functools
import math

import jax
import jax.numpy as jnp
from jax import lax
from jax.experimental import pallas as pl
from jax.experimental.pallas import tpu as pltpu
from jax.sharding import PartitionSpec as P

ROPE_THETA = 10000.0
YARN_FACTOR = 40.0
ORIG_CTX = 4096.0
BETA_FAST = 32.0
BETA_SLOW = 1.0
NORM_EPS = 1e-6

MESH = pl.DeviceIdType.MESH
F32 = jnp.float32
BF16 = jnp.bfloat16


def rope_freqs(rot_dim):
    half_dim = rot_dim // 2
    log_base = 2.0 * math.log(ROPE_THETA)
    low_idx = max(math.floor(rot_dim * math.log(ORIG_CTX / (BETA_FAST * 2.0 * math.pi)) / log_base), 0)
    high_idx = min(math.ceil(rot_dim * math.log(ORIG_CTX / (BETA_SLOW * 2.0 * math.pi)) / log_base), half_dim - 1)
    spread = max(high_idx - low_idx, 0.001)
    freq_list = []
    for freq_idx in range(half_dim):
        base_freq = ROPE_THETA ** (-2.0 * freq_idx / rot_dim)
        ramp_val = min(max((freq_idx - low_idx) / spread, 0.0), 1.0)
        freq_list.append(base_freq / YARN_FACTOR * ramp_val + base_freq * (1.0 - ramp_val))
    return jnp.asarray(freq_list, dtype=jnp.float32)


def rotate_half(act_in, cos_t, sin_t):
    half_dim = act_in.shape[-1] // 2
    first = act_in[..., :half_dim]
    second = act_in[..., half_dim:]
    return jnp.concatenate([first * cos_t - second * sin_t, second * cos_t + first * sin_t], axis=-1)


def rms_norm(act_in, gain):
    mean_sq = jnp.mean(act_in * act_in, axis=-1, keepdims=True)
    return act_in * lax.rsqrt(mean_sq + NORM_EPS) * gain


def dot(a, b):
    return jnp.dot(a, b, preferred_element_type=F32)


def mla_kernel(cfg, cblk, cqT, trig, wq, wk, wv, wo, out,
               c_all, cq_all, trig_all, cT, kcat, vT, q_scr, o_all, acc_o, acc, stage, fin,
               wq_buf, wk_buf, wv_buf, wo_buf,
               sendR, recvR, sendL, recvL, sendD, recvD, sendX, recvX, send_o, recv_o, send_f, recv_f,
               wq_sem, wk_sem, wv_sem, wo_sem):
    Z, T, C, NOPE, ROPE, V, H = cfg["Z"], cfg["T"], cfg["C"], cfg["NOPE"], cfg["ROPE"], cfg["V"], cfg["H"]
    CH, HB, D, scale2 = cfg["CH"], cfg["HB"], cfg["D"], cfg["scale2"]
    NQB, NOB = wq_buf.shape[0], wo_buf.shape[0]
    HC = H // 2
    NU = HC // 2
    DC = D // 2
    W = 2 * T
    QK = NOPE + ROPE
    half = ROPE // 2
    NR, NL = Z // 2, (Z - 1) // 2

    idx = lax.axis_index("sp")
    z, core = idx // 2, lax.rem(idx, 2)
    right = lax.rem(z + 1, Z) * 2 + core
    left = lax.rem(z + Z - 1, Z) * 2 + core
    other = z * 2 + (1 - core)

    def rows_of(chip_off):
        blk = lax.rem(z + chip_off + 2 * Z, Z) * 2 + core
        return pl.ds(pl.multiple_of(blk * T, T), T)

    barrier = pltpu.get_barrier_semaphore()
    for dev in (left, right, other):
        pl.semaphore_signal(barrier, inc=1, device_id={"sp": dev}, device_id_type=MESH)
    pl.semaphore_wait(barrier, 3)

    def remote(src, dst, ssem, rsem, dev):
        return pltpu.make_async_remote_copy(src_ref=src, dst_ref=dst, send_sem=ssem, recv_sem=rsem,
                                            device_id={"sp": dev}, device_id_type=MESH)

    own = rows_of(0)

    def right_copy(s):
        rows = rows_of(-s)
        return remote(cblk if s == 0 else c_all.at[rows], c_all.at[rows], sendR.at[s], recvR.at[s], right)

    def left_copy(s):
        rows = rows_of(s)
        return remote(cblk if s == 0 else c_all.at[rows], c_all.at[rows], sendL.at[s], recvL.at[s], left)

    def pair_copy(s):
        if s == 0:
            rows, src = own, cblk
        else:
            rows = rows_of(-s) if s <= NR else rows_of(s - NR)
            src = c_all.at[rows]
        return remote(src, c_all.at[rows], sendD.at[s], recvD.at[s], other)

    cq_copy = remote(cqT, cq_all.at[core], sendX.at[0], recvX.at[0], other)
    trig_copy = remote(trig, trig_all.at[core], sendX.at[1], recvX.at[1], other)
    cq_copy.start()
    trig_copy.start()
    right_copy(0).start()
    left_copy(0).start()
    pair_copy(0).start()

    def wq_copy(u):
        h0 = core * HC + 2 * u
        return pltpu.make_async_copy(wq.at[pl.ds(h0, 2)], wq_buf.at[lax.rem(u, NQB)], wq_sem.at[lax.rem(u, NQB)])

    def wkv_copies(u):
        h0 = core * HC + 2 * u
        p = lax.rem(u, 2)
        return (pltpu.make_async_copy(wk.at[pl.ds(h0, 2)], wk_buf.at[p], wk_sem.at[p]),
                pltpu.make_async_copy(wv.at[pl.ds(h0, 2)], wv_buf.at[p], wv_sem.at[p]))

    def wo_copy(i):
        hb = lax.rem(core * (HC // HB) + i, H // HB)
        src = wo.at[pl.ds(pl.multiple_of(hb * HB * V, HB * V), HB * V), pl.ds(pl.multiple_of(core * DC, DC), DC)]
        return pltpu.make_async_copy(src, wo_buf.at[lax.rem(i, NOB)], wo_sem.at[lax.rem(i, NOB)])

    for u in range(min(NQB, NU)):
        wq_copy(u).start()

    c_all[own, :] = cblk[...]
    cq_all[core] = cqT[...]
    trig_all[core] = trig[...]
    cq_copy.wait_recv()
    trig_copy.wait_recv()

    cosT = jnp.concatenate([trig_all[0, :half], trig_all[1, :half]], axis=1)
    sinT = jnp.concatenate([trig_all[0, half:], trig_all[1, half:]], axis=1)

    def q_unit(u, carry):
        slot = lax.rem(u, NQB)
        wq_copy(u).wait()
        w2 = wq_buf[slot].reshape(2 * QK, wq_buf.shape[3])
        cqs = jnp.concatenate([cq_all[0], cq_all[1]], axis=1)
        q = dot(w2, cqs)
        for h in range(2):
            b = h * QK
            z1, z2 = q[b + NOPE:b + NOPE + half], q[b + NOPE + half:b + QK]
            q_scr[u, h, :NOPE] = q[b:b + NOPE].astype(BF16)
            q_scr[u, h, NOPE:NOPE + half] = (z1 * cosT - z2 * sinT).astype(BF16)
            q_scr[u, h, NOPE + half:QK] = (z2 * cosT + z1 * sinT).astype(BF16)
            q_scr[u, h, QK:] = jnp.zeros((q_scr.shape[2] - QK, W), BF16)

        @pl.when(u + NQB < NU)
        def _():
            wq_copy(u + NQB).start()
        return carry

    cuts = [NU * s // NR for s in range(NR + 1)]
    for s in range(NR):
        lax.fori_loop(cuts[s], cuts[s + 1], q_unit, 0)
        right_copy(s).wait_recv()
        if s + 1 < NR:
            right_copy(s + 1).start()
        pair_copy(s + 1).start()
        if s < NL:
            left_copy(s).wait_recv()
            if s + 1 < NL:
                left_copy(s + 1).start()
            pair_copy(1 + NR + s).start()

    for c in wkv_copies(0) + wkv_copies(1):
        c.start()
    for i in range(NOB):
        wo_copy(i).start()
    for s in range(1 + NR + NL):
        pair_copy(s).wait_recv()

    nch = (W * z) // CH + 1

    def transpose_chunk(j, carry):
        cT[j] = c_all[pl.ds(pl.multiple_of(j * CH, CH), CH), :C].T
        return carry

    lax.fori_loop(0, nch, transpose_chunk, 0)

    def make_kv(u, j, slot):
        p = lax.rem(u, 2)
        cc = c_all[pl.ds(pl.multiple_of(j * CH, CH), CH), :C]
        pe = c_all[pl.ds(pl.multiple_of(j * CH, CH), CH), C:]
        k2 = dot(cc, jnp.concatenate([wk_buf[p, 0], wk_buf[p, 1]], axis=1)).astype(BF16)
        for h in range(2):
            kcat[slot, h, :, :NOPE] = k2[:, h * NOPE:(h + 1) * NOPE]
            kcat[slot, h, :, NOPE:] = pe
        vT[slot] = dot(wv_buf[p].reshape(2 * V, C), cT[j]).astype(BF16)

    def body(u, j, t, un, jn, ml, masked):
        slot, nslot = lax.rem(t, 2), lax.rem(t + 1, 2)
        s = [dot(kcat[slot, h], q_scr[u, h]) for h in range(2)]
        make_kv(un, jn, nslot)
        out = []
        for h in range(2):
            m, l = ml[h]
            sh = s[h]
            if masked:
                kk = lax.broadcasted_iota(jnp.int32, (CH, W), 0)
                qq = lax.broadcasted_iota(jnp.int32, (CH, W), 1)
                sh = jnp.where(kk - qq <= W * z - CH * j, sh, -jnp.inf)
            mn = jnp.maximum(m, jnp.max(sh, axis=0, keepdims=True))
            alpha = jnp.exp2((m - mn) * scale2)
            p = jnp.exp2((sh - mn) * scale2)
            ln = l * alpha + jnp.sum(p, axis=0, keepdims=True)
            acc_o[h] = acc_o[h] * alpha + dot(vT[slot, h * V:(h + 1) * V], p.astype(BF16))
            out.append((mn, ln))
        return tuple(out)

    def o_copy(u):
        unit = core * NU + u
        return remote(o_all.at[unit], o_all.at[unit], send_o.at[u], recv_o.at[u], other)

    for c in wkv_copies(0):
        c.wait()
    make_kv(0, 0, 0)

    def attn_unit(u, carry):
        t0 = u * nch
        acc_o[...] = jnp.zeros(acc_o.shape, F32)
        init = tuple((jnp.full((1, W), -1e30, F32), jnp.zeros((1, W), F32)) for _ in range(2))
        ml = lax.fori_loop(0, nch - 1, lambda j, ml: body(u, j, t0 + j, u, j + 1, ml, False), init)

        @pl.when(u + 1 < NU)
        def _():
            for c in wkv_copies(u + 1):
                c.wait()

        @pl.when(u + 2 < NU)
        def _():
            for c in wkv_copies(u + 2):
                c.start()

        @pl.when(u > 0)
        def _():
            o_copy(u - 1).start()

        ml = body(u, nch - 1, t0 + nch - 1, lax.rem(u + 1, NU), 0, ml, True)
        for h in range(2):
            o_all[core * NU + u, :, h * V:(h + 1) * V] = (acc_o[h] * (1.0 / ml[h][1])).T.astype(BF16)
        return carry

    lax.fori_loop(0, NU, attn_unit, 0)

    NB = H // HB
    CT = DC // 5 if DC % 640 == 0 else DC

    def out_block(i, first):
        hb = lax.rem(core * (HC // HB) + i, NB)
        slot = lax.rem(i, NOB)
        wo_copy(i).wait()
        ob = jnp.concatenate([o_all[hb * (HB // 2) + g] for g in range(HB // 2)], axis=1)
        for r in range(DC // CT):
            cs = slice(r * CT, (r + 1) * CT)
            d = dot(ob, wo_buf[slot, :, cs])
            if first:
                acc[:, cs] = d
            else:
                acc[:, cs] = acc[:, cs] + d

        @pl.when(i + NOB < NB)
        def _():
            wo_copy(i + NOB).start()

    out_block(0, True)
    o_copy(NU - 1).start()

    def own_block(i, carry):
        out_block(i, False)
        return carry

    def far_block(i, carry):
        for g in range(HB // 2):
            o_copy((i - NB // 2) * (HB // 2) + g).wait_recv()
        out_block(i, False)
        return carry

    lax.fori_loop(1, NB // 2, own_block, 0)
    lax.fori_loop(NB // 2, NB, far_block, 0)

    stage[...] = acc[pl.ds(pl.multiple_of((1 - core) * T, T), T), :].astype(BF16)
    final = remote(stage, fin, send_f, recv_f, other)
    final.start()
    out[:, pl.ds(pl.multiple_of(core * DC, DC), DC)] = acc[pl.ds(pl.multiple_of(core * T, T), T), :].astype(BF16)
    final.wait_recv()
    out[:, pl.ds(pl.multiple_of((1 - core) * DC, DC), DC)] = fin[...]

    for s in range(NR):
        right_copy(s).wait_send()
    for s in range(NL):
        left_copy(s).wait_send()
    for s in range(1 + NR + NL):
        pair_copy(s).wait_send()
    cq_copy.wait_send()
    trig_copy.wait_send()

    def drain(u, carry):
        o_copy(u).wait_send()
        return carry

    lax.fori_loop(0, NU, drain, 0)
    final.wait_send()


def solution(mesh):
    groups = mesh.shape["sp"]
    tok_spec = P(("dp", "sp"))
    rows_spec = P(("dp", "sp"), None)
    rep = P()

    def local_step(tok_in, tok_pos, w_dq, g_q, w_uq, w_dkv, g_kv, w_uk, w_uv, w_o):
        T, D = tok_in.shape
        CQ, H, QK = w_uq.shape
        C = g_kv.shape[0]
        ROPE = w_dkv.shape[1] - C
        NOPE = QK - ROPE
        V = w_uv.shape[2]
        Z = groups // 2
        seq = T * groups
        W = 2 * T
        CH = 2 * W
        HB = min(8, H // 2)
        NU = H // 4
        NCH = seq // CH
        KD = 2 * NOPE
        attn_scale = (0.1 * math.log(YARN_FACTOR) + 1.0) ** 2 / math.sqrt(QK)

        angles = tok_pos.astype(F32)[:, None] * rope_freqs(ROPE)[None, :]
        cos_t = jnp.cos(angles)
        sin_t = jnp.sin(angles)
        q_lat = rms_norm(jnp.dot(tok_in, w_dq, preferred_element_type=F32), g_q).astype(BF16)
        kv_lat = jnp.dot(tok_in, w_dkv, preferred_element_type=F32)
        cache_kv = rms_norm(kv_lat[:, :C], g_kv).astype(BF16)
        cache_pe = rotate_half(kv_lat[:, C:], cos_t, sin_t).astype(BF16)

        cblk = jnp.concatenate([cache_kv, cache_pe, jnp.zeros((T, KD - NOPE - ROPE), BF16)], axis=1)
        trig = jnp.concatenate([cos_t.T, sin_t.T], axis=0)
        cfg = dict(Z=Z, T=T, C=C, NOPE=NOPE, ROPE=ROPE, V=V, H=H, CH=CH, HB=HB, D=D, scale2=attn_scale * math.log2(math.e))
        NQB, NOB = 4, min(4, H // HB)
        NR, NL = Z // 2, (Z - 1) // 2
        dma = pltpu.SemaphoreType.DMA
        vm = pl.BlockSpec(memory_space=pltpu.VMEM)
        hbm = pl.BlockSpec(memory_space=pltpu.HBM)
        attn_out = pl.pallas_call(
            functools.partial(mla_kernel, cfg),
            out_shape=jax.ShapeDtypeStruct((T, D), BF16),
            in_specs=[vm, vm, vm, hbm, hbm, hbm, hbm],
            out_specs=vm,
            scratch_shapes=[
                pltpu.VMEM((seq, C + KD - NOPE), BF16),
                pltpu.VMEM((2, CQ, T), BF16),
                pltpu.VMEM((2, ROPE, T), F32),
                pltpu.VMEM((NCH, C, CH), BF16),
                pltpu.VMEM((2, 2, CH, KD), BF16),
                pltpu.VMEM((2, 2 * V, CH), BF16),
                pltpu.VMEM((NU, 2, KD, W), BF16),
                pltpu.VMEM((H // 2, W, 2 * V), BF16),
                pltpu.VMEM((2, V, W), F32),
                pltpu.VMEM((W, D // 2), F32),
                pltpu.VMEM((T, D // 2), BF16),
                pltpu.VMEM((T, D // 2), BF16),
                pltpu.VMEM((NQB, 2, QK, CQ), BF16),
                pltpu.VMEM((2, 2, C, NOPE), BF16),
                pltpu.VMEM((2, 2, V, C), BF16),
                pltpu.VMEM((NOB, HB * V, D // 2), BF16),
                dma((NR,)), dma((NR,)), dma((max(NL, 1),)), dma((max(NL, 1),)), dma((1 + NR + NL,)), dma((1 + NR + NL,)),
                dma((2,)), dma((2,)), dma((NU,)), dma((NU,)), dma, dma,
                dma((NQB,)), dma((2,)), dma((2,)), dma((NOB,)),
            ],
            compiler_params=pltpu.CompilerParams(collective_id=0, has_side_effects=True, vmem_limit_bytes=66_000_000),
            name="mla",
        )(cblk, q_lat.T, trig, jnp.transpose(w_uq, (1, 2, 0)), jnp.transpose(w_uk, (1, 0, 2)),
          jnp.transpose(w_uv, (1, 2, 0)), w_o.reshape(H * V, D))
        return attn_out, cache_kv, cache_pe

    return jax.shard_map(local_step, mesh=mesh, in_specs=(rows_spec, tok_spec) + (rep,) * 8,
                         out_specs=(rows_spec, rows_spec, rows_spec), check_vma=False)
```
